8 devices in a mesh: dp: 2 (over z, y), vp: 4 (over x, core).
Axes of the slice: x: 2, y: 2, z: 1, core: 2. Of those that a mesh axis runs over, the one named last changes fastest.
Arguments:
- hidden: bfloat16 [512, 12288], P('dp'), parts along dimension 0
- w_head: bfloat16 [12288, 32768], P(None, 'vp')
- inv_temp: float32 [512], P('dp'), parts along dimension 0
- target_ids: int32 [512], P('dp'), parts along dimension 0
Outputs:
- output 1: float32 [512, 32768], P(('dp', 'vp')), parts along dimension 0
- output 2: float32 [512], P('dp'), parts along dimension 0
There are 2 independent parts. The reference program is written for one: setup_inputs(seed, part) draws one part's arguments, and reference() takes and returns one part's arrays. A program takes and returns all parts, laid end to end along the dimension named above; an argument that names none is the same for every part.
All inputs are finite; a program needn't handle non-finite values.
Results may differ from the reference program's by a relative error of at most 0.001.
Values are sent between devices in bfloat16 or wider.
A program may use at most 1 GiB of HBM per device.

```python
import math
import jax
import jax.numpy as jnp
from jax import lax

BATCH = 256
HIDDEN = 12288
VOCAB = 32768
W_ROW_BLOCK = 256


def draw_head(key, direction, profile):
    num_blocks = HIDDEN // W_ROW_BLOCK
    dir_blocks = direction.reshape(num_blocks, W_ROW_BLOCK)

    def one_block(block_args):
        block_idx, dir_rows = block_args
        noise_rows = jax.random.normal(jax.random.fold_in(key, block_idx), (W_ROW_BLOCK, VOCAB), jnp.float32)
        head_rows = (noise_rows + dir_rows[:, None] * profile[None, :]) * (HIDDEN ** -0.5)
        return head_rows.astype(jnp.bfloat16)

    blocks = lax.map(one_block, (jnp.arange(num_blocks), dir_blocks))
    return blocks.reshape(HIDDEN, VOCAB)


def setup_inputs(seed: int = 0, part: int = 0) -> dict:
    base_key = jax.random.key(seed)
    shared_key = jax.random.fold_in(base_key, 1)
    part_key = jax.random.fold_in(jax.random.fold_in(base_key, 2), part)
    key_dir, key_head = jax.random.split(shared_key)
    key_hid, key_gain, key_temp, key_ids = jax.random.split(part_key, 4)
    direction = jax.random.normal(key_dir, (HIDDEN,), jnp.float32)
    vocab_pos = jnp.arange(VOCAB, dtype=jnp.float32) / VOCAB
    profile = 1.5 * jnp.exp(-8.0 * vocab_pos)
    w_head = draw_head(key_head, direction, profile)
    row_gain = 2.0 + 0.5 * jax.random.normal(key_gain, (BATCH, 1), jnp.float32)
    hidden = jax.random.normal(key_hid, (BATCH, HIDDEN), jnp.float32) + row_gain * direction[None, :] * (HIDDEN ** -0.5)
    row_pos = jnp.arange(BATCH)
    log_temp = jax.random.uniform(key_temp, (BATCH,), jnp.float32, minval=math.log(0.5), maxval=math.log(32.0))
    inv_temp = jnp.where(row_pos == 0, 32.0, jnp.exp(log_temp))
    target_ids = jax.random.randint(key_ids, (BATCH,), 0, VOCAB, dtype=jnp.int32)
    target_ids = jnp.where(row_pos == 1, VOCAB - 1, target_ids)
    return {"hidden": hidden.astype(jnp.bfloat16), "w_head": w_head, "inv_temp": inv_temp, "target_ids": target_ids}


def reference(hidden, w_head, inv_temp, target_ids):
    logits = jnp.dot(hidden, w_head, preferred_element_type=jnp.float32)
    scaled = logits * inv_temp[:, None]
    row_max = jnp.max(scaled, axis=1, keepdims=True)
    exp_vals = jnp.exp(scaled - row_max)
    probabilities = exp_vals / jnp.sum(exp_vals, axis=1, keepdims=True)
    cdf_table = jnp.cumsum(probabilities, axis=1)
    cdf_at_target = jnp.take_along_axis(cdf_table, target_ids[:, None], axis=1)[:, 0]
    return cdf_table, cdf_at_target
```

```python
import functools
import jax
import jax.numpy as jnp
from jax import lax
from jax.experimental import pallas as pl
from jax.experimental.pallas import tpu as pltpu
from jax.sharding import PartitionSpec as P

TILE = 256
K_CHUNK = 3072
PACE = (3, 4)
GROUP = 4
MESH = pl.DeviceIdType.MESH


def head_kernel(
    n_vp, rows, n_tiles, n_k,
    h_hbm, w_hbm, temp_ref, tgt_ref,
    tab_ref, cdf_ref,
    h_buf, w_buf, stage, acc, temp_b, tgt_b, m_l, s_l, g_l, st_out, st_in, col_b, tri,
    h_sem, w_sem, send_sem, recv_sem, st_send, st_recv,
):
    dp = lax.axis_index("dp")
    me = lax.axis_index("vp")
    batch = n_vp * rows
    local_vocab = n_tiles * TILE
    chip = me // 2
    mate = chip * 2 + lax.rem(me + 1, 2)
    far0 = (1 - chip) * 2 + lax.rem(me, 2)
    far1 = (1 - chip) * 2 + lax.rem(me + 1, 2)

    barrier = pltpu.get_barrier_semaphore()
    for peer in (mate, far0, far1):
        pl.semaphore_signal(barrier, inc=1, device_id=(dp, peer), device_id_type=MESH)

    def w_copy(t, kc):
        slot = lax.rem(t, 2) * n_k + kc
        return pltpu.make_async_copy(
            w_hbm.at[pl.ds(kc * K_CHUNK, K_CHUNK), pl.ds(pl.multiple_of(t * TILE, TILE), TILE)],
            w_buf.at[slot], w_sem.at[slot])

    def h_copy(kc):
        return pltpu.make_async_copy(
            h_hbm.at[:, pl.ds(kc * K_CHUNK, K_CHUNK)], h_buf.at[:, pl.ds(kc * K_CHUNK, K_CHUNK)], h_sem.at[kc])

    for kc in range(n_k):
        w_copy(0, kc).start()
        h_copy(kc).start()
    for kc in range(n_k):
        w_copy(1, kc).start()

    temp_b[...] = jnp.broadcast_to(temp_ref[...], (128, batch)).T
    tgt_b[...] = jnp.broadcast_to(tgt_ref[...].astype(jnp.float32), (128, batch)).T
    m_l[...] = jnp.full_like(m_l, -jnp.inf)
    s_l[...] = jnp.zeros_like(s_l)
    g_l[...] = jnp.zeros_like(g_l)
    r_id = lax.broadcasted_iota(jnp.int32, (TILE, TILE), 0)
    c_id = lax.broadcasted_iota(jnp.int32, (TILE, TILE), 1)
    upper = jnp.where(r_id <= c_id, 1.0, 0.0).astype(jnp.bfloat16)
    for q in range(3):
        tri[q * TILE:(q + 1) * TILE, :] = upper

    def send(t, peer, k):
        return pltpu.make_async_remote_copy(
            src_ref=stage.at[t, pl.ds(pl.multiple_of(peer * rows, rows), rows), :],
            dst_ref=tab_ref.at[:, pl.ds(pl.multiple_of(me * local_vocab + t * TILE, TILE), TILE)],
            send_sem=send_sem.at[k, t],
            recv_sem=recv_sem.at[me, t],
            device_id=(dp, peer), device_id_type=MESH)

    def recv(t, src):
        cols = tab_ref.at[:, pl.ds(pl.multiple_of(src * local_vocab + t * TILE, TILE), TILE)]
        return pltpu.make_async_remote_copy(
            src_ref=cols, dst_ref=cols, send_sem=send_sem.at[0, t], recv_sem=recv_sem.at[src, t],
            device_id=(dp, src), device_id_type=MESH)

    def send_far(t):
        send(t, far0, 1).start()
        send(t, far1, 2).start()

    def tile(t, first):
        for kc in range(n_k):
            if first:
                h_copy(kc).wait()
            w_copy(t, kc).wait()
            slot = lax.rem(t, 2) * n_k + kc
            part = jnp.dot(h_buf[:, kc * K_CHUNK:(kc + 1) * K_CHUNK], w_buf[slot],
                           preferred_element_type=jnp.float32)
            if kc == 0:
                acc[...] = part
            elif kc < n_k - 1:
                acc[...] += part
            else:
                total = acc[...] + part

            if first:
                w_copy(t + 2, kc).start()
            else:
                @pl.when(t + 2 < n_tiles)
                def _():
                    w_copy(t + 2, kc).start()
        temp = temp_b[...]
        z0 = total[:, :128] * temp
        z1 = total[:, 128:] * temp
        stage[t, :, :128] = z0
        stage[t, :, 128:] = z1
        m_old = m_l[...]
        m_new = jnp.maximum(m_old, jnp.maximum(z0, z1))
        keep = jnp.exp(m_old - m_new)
        e0 = jnp.exp(z0 - m_new)
        e1 = jnp.exp(z1 - m_new)
        base = (me * local_vocab + t * TILE).astype(jnp.float32)
        dist = tgt_b[...] - base
        lane = lax.broadcasted_iota(jnp.int32, (batch, 128), 1).astype(jnp.float32)
        m_l[...] = m_new
        s_l[...] = s_l[...] * keep + (e0 + e1)
        g_l[...] = g_l[...] * keep + (jnp.where(lane <= dist, e0, 0.0) + jnp.where(lane + 128.0 <= dist, e1, 0.0))

    tile(jnp.int32(0), True)
    pl.semaphore_wait(barrier, n_vp - 1)
    send_far(0)
    send(0, mate, 0).start()

    num, den = PACE

    def step(t, carry):
        tile(t, False)
        now, before = (t * num) // den, ((t - 1) * num) // den

        @pl.when(now > before)
        def _():
            send_far(now)
        send(t, mate, 0).start()
        return carry

    lax.fori_loop(1, n_tiles, step, 0)

    m_lane = m_l[...]
    m_dev = jnp.max(m_lane, axis=1, keepdims=True)
    w_lane = jnp.exp(m_lane - m_dev)
    s_dev = jnp.sum(s_l[...] * w_lane, axis=1, keepdims=True)
    g_dev = jnp.sum(g_l[...] * w_lane, axis=1, keepdims=True)
    lane = lax.broadcasted_iota(jnp.int32, (batch, 128), 1)
    packed = jnp.where(lane == 0, m_dev, jnp.where(lane == 1, s_dev, jnp.where(lane == 2, g_dev, 0.0)))
    stats = packed.T[:8, :]
    st_out[...] = stats
    st_in[me] = stats

    def st_copy(peer, k):
        return pltpu.make_async_remote_copy(
            src_ref=st_out, dst_ref=st_in.at[me], send_sem=st_send.at[k], recv_sem=st_recv.at[me],
            device_id=(dp, peer), device_id_type=MESH)

    def st_wait(src):
        pltpu.make_async_remote_copy(
            src_ref=st_out, dst_ref=st_in.at[src], send_sem=st_send.at[0], recv_sem=st_recv.at[src],
            device_id=(dp, src), device_id_type=MESH).wait_recv()

    peers = ((far0, 1), (far1, 2), (mate, 0))
    for peer, k in peers:
        st_copy(peer, k).start()
    for t in range(((n_tiles - 1) * num) // den + 1, n_tiles):
        send_far(t)
    for peer, k in peers:
        st_wait(peer)

    everyone = [st_in[i] for i in range(n_vp)]
    m_all = functools.reduce(jnp.maximum, [x[0:1] for x in everyone])
    weight = [jnp.exp(x[0:1] - m_all) for x in everyone]
    s_w = [x[1:2] * w for x, w in zip(everyone, weight)]
    inv = 1.0 / functools.reduce(jnp.add, s_w)
    cdf_ref[...] = functools.reduce(jnp.add, [x[2:3] * w for x, w in zip(everyone, weight)]) * inv
    offsets, running = [], jnp.zeros_like(inv)
    for x in s_w:
        offsets.append(running * inv)
        running = running + x
    sub = lax.broadcasted_iota(jnp.int32, (128, batch), 0)
    table = jnp.zeros((128, batch), jnp.float32)
    for i, row in enumerate([m_all, inv] + offsets):
        table = jnp.where(sub == i, row, table)
    col_b[...] = table.T
    mine = col_b[pl.ds(pl.multiple_of(me * rows, rows), rows), :]
    m_col, inv_col = mine[:, 0:1], mine[:, 1:2]
    lane_r = lax.broadcasted_iota(jnp.int32, (rows, 128), 1)

    def offset(src):
        return jnp.sum(jnp.where(lane_r == src + 2, mine, 0.0), axis=1, keepdims=True)

    def finish(src, g, carry, own):
        parts = []
        for q in range(GROUP):
            t = g * GROUP + q
            if own:
                z = stage[t, pl.ds(pl.multiple_of(me * rows, rows), rows), :]
            else:
                recv(t, src).wait_recv()
                z = tab_ref[:, pl.ds(pl.multiple_of(src * local_vocab + t * TILE, TILE), TILE)]
            parts.append(jnp.exp(z - m_col) * inv_col)
        p = jnp.concatenate(parts, axis=0)
        hi = p.astype(jnp.bfloat16)
        rest = p - hi.astype(jnp.float32)
        mid = rest.astype(jnp.bfloat16)
        low = (rest - mid.astype(jnp.float32)).astype(jnp.bfloat16)
        c = jnp.dot(jnp.concatenate([hi, mid, low], axis=1), tri[...], preferred_element_type=jnp.float32)
        for q in range(GROUP):
            t = g * GROUP + q
            cq = c[q * rows:(q + 1) * rows, :]
            tab_ref[:, pl.ds(pl.multiple_of(src * local_vocab + t * TILE, TILE), TILE)] = cq + carry
            carry = carry + cq[:, TILE - 1:TILE]
        return carry

    n_groups = n_tiles // GROUP
    lax.fori_loop(0, n_groups, lambda g, c: finish(me, g, c, True), offset(me))
    lax.fori_loop(0, n_groups, lambda g, c: finish(mate, g, c, False), offset(mate))
    lax.fori_loop(0, n_groups, lambda g, c: (finish(far0, g, c[0], False), finish(far1, g, c[1], False)),
                  (offset(far0), offset(far1)))

    def drain(t, carry):
        for peer, k in peers:
            send(t, peer, k).wait_send()
        return carry

    lax.fori_loop(0, n_tiles, drain, 0)
    for peer, k in peers:
        st_copy(peer, k).wait_send()


def solution(mesh):
    n_vp = mesh.shape["vp"]

    def local_step(hidden, w_local, inv_temp, target_ids):
        batch, depth = hidden.shape
        rows = batch // n_vp
        local_vocab = w_local.shape[1]
        n_tiles, n_k = local_vocab // TILE, depth // K_CHUNK
        f32 = jnp.float32
        vmem = pl.BlockSpec(memory_space=pltpu.VMEM)
        hbm = pl.BlockSpec(memory_space=pl.ANY)
        table, at_target = pl.pallas_call(
            functools.partial(head_kernel, n_vp, rows, n_tiles, n_k),
            out_shape=(pltpu.VMEM((rows, n_vp * local_vocab), f32),
                       jax.ShapeDtypeStruct((1, batch), f32)),
            in_specs=[hbm, hbm, vmem, vmem],
            out_specs=(vmem, vmem),
            scratch_shapes=[
                pltpu.VMEM((batch, depth), jnp.bfloat16),
                pltpu.VMEM((2 * n_k, K_CHUNK, TILE), jnp.bfloat16),
                pltpu.VMEM((n_tiles, batch, TILE), f32),
                pltpu.VMEM((batch, TILE), f32),
                pltpu.VMEM((batch, 128), f32),
                pltpu.VMEM((batch, 128), f32),
                pltpu.VMEM((batch, 128), f32),
                pltpu.VMEM((batch, 128), f32),
                pltpu.VMEM((batch, 128), f32),
                pltpu.VMEM((8, batch), f32),
                pltpu.VMEM((n_vp, 8, batch), f32),
                pltpu.VMEM((batch, 128), f32),
                pltpu.VMEM((3 * TILE, TILE), jnp.bfloat16),
                pltpu.SemaphoreType.DMA((n_k,)),
                pltpu.SemaphoreType.DMA((2 * n_k,)),
                pltpu.SemaphoreType.DMA((3, n_tiles)),
                pltpu.SemaphoreType.DMA((n_vp, n_tiles)),
                pltpu.SemaphoreType.DMA((3,)),
                pltpu.SemaphoreType.DMA((n_vp,)),
            ],
            compiler_params=pltpu.CompilerParams(
                collective_id=0, has_side_effects=True, vmem_limit_bytes=38 * 2**20),
        )(hidden, w_local, inv_temp[None, :], target_ids[None, :])
        return table, at_target[0]

    return jax.shard_map(
        local_step,
        mesh=mesh,
        in_specs=(P("dp", None), P(None, "vp"), P("dp"), P("dp")),
        out_specs=(P(("dp", "vp"), None), P("dp")),
        check_vma=False,
    )
```

```python
import functools
import jax
import jax.numpy as jnp
from jax import lax
from jax.experimental import pallas as pl
from jax.experimental.pallas import tpu as pltpu
from jax.sharding import PartitionSpec as P

TILE = 256
SLOTS = 3
PIECES = 4
PACE = (3, 4)
GROUP = 4
MESH = pl.DeviceIdType.MESH


def head_kernel(
    n_vp, rows, n_tiles,
    h_hbm, w_hbm, temp_ref, tgt_ref,
    tab_ref, cdf_ref,
    h_buf, w_buf, stage, temp_b, tgt_b, m_l, s_l, g_l, st_out, st_in, col_b, tri,
    h_sem, w0_sem, w_sem, send_sem, recv_sem, st_send, st_recv,
):
    dp = lax.axis_index("dp")
    me = lax.axis_index("vp")
    batch = n_vp * rows
    local_vocab = n_tiles * TILE
    chip = me // 2
    mate = chip * 2 + lax.rem(me + 1, 2)
    far0 = (1 - chip) * 2 + lax.rem(me, 2)
    far1 = (1 - chip) * 2 + lax.rem(me + 1, 2)

    barrier = pltpu.get_barrier_semaphore()
    for peer in (mate, far0, far1):
        pl.semaphore_signal(barrier, inc=1, device_id=(dp, peer), device_id_type=MESH)

    depth = h_buf.shape[1]
    piece = depth // PIECES

    def w_copy(t):
        slot = lax.rem(t, SLOTS)
        return pltpu.make_async_copy(
            w_hbm.at[:, pl.ds(pl.multiple_of(t * TILE, TILE), TILE)], w_buf.at[slot], w_sem.at[slot])

    def first_copies(i):
        span = pl.ds(i * piece, piece)
        return (pltpu.make_async_copy(w_hbm.at[span, pl.ds(0, TILE)], w_buf.at[0, span, :], w0_sem.at[i]),
                pltpu.make_async_copy(h_hbm.at[:, span], h_buf.at[:, span], h_sem.at[i]))

    for i in range(PIECES):
        for copy in first_copies(i):
            copy.start()
    for t in range(1, SLOTS):
        w_copy(jnp.int32(t)).start()

    temp_b[...] = jnp.broadcast_to(temp_ref[...], (128, batch)).T
    tgt_b[...] = jnp.broadcast_to(tgt_ref[...].astype(jnp.float32), (128, batch)).T
    m_l[...] = jnp.full_like(m_l, -jnp.inf)
    s_l[...] = jnp.zeros_like(s_l)
    g_l[...] = jnp.zeros_like(g_l)
    r_id = lax.broadcasted_iota(jnp.int32, (TILE, TILE), 0)
    c_id = lax.broadcasted_iota(jnp.int32, (TILE, TILE), 1)
    upper = jnp.where(r_id <= c_id, 1.0, 0.0).astype(jnp.bfloat16)
    for q in range(3):
        tri[q * TILE:(q + 1) * TILE, :] = upper

    def send(t, peer, k):
        return pltpu.make_async_remote_copy(
            src_ref=stage.at[t, pl.ds(pl.multiple_of(peer * rows, rows), rows), :],
            dst_ref=tab_ref.at[:, pl.ds(pl.multiple_of(me * local_vocab + t * TILE, TILE), TILE)],
            send_sem=send_sem.at[k, t],
            recv_sem=recv_sem.at[me, t],
            device_id=(dp, peer), device_id_type=MESH)

    def recv(t, src):
        cols = tab_ref.at[:, pl.ds(pl.multiple_of(src * local_vocab + t * TILE, TILE), TILE)]
        return pltpu.make_async_remote_copy(
            src_ref=cols, dst_ref=cols, send_sem=send_sem.at[0, t], recv_sem=recv_sem.at[src, t],
            device_id=(dp, src), device_id_type=MESH)

    def send_far(t):
        send(t, far0, 1).start()
        send(t, far1, 2).start()

    def tile(t, first):
        if first:
            for i in range(PIECES):
                for copy in first_copies(i):
                    copy.wait()
                part = jnp.dot(h_buf[:, i * piece:(i + 1) * piece], w_buf[0, i * piece:(i + 1) * piece, :],
                               preferred_element_type=jnp.float32)
                total = part if i == 0 else total + part
            w_copy(t + SLOTS).start()
        else:
            w_copy(t).wait()
            total = jnp.dot(h_buf[...], w_buf[lax.rem(t, SLOTS)], preferred_element_type=jnp.float32)

            @pl.when(t + SLOTS < n_tiles)
            def _():
                w_copy(t + SLOTS).start()
        temp = temp_b[...]
        z0 = total[:, :128] * temp
        z1 = total[:, 128:] * temp
        stage[t, :, :128] = z0
        stage[t, :, 128:] = z1
        m_old = m_l[...]
        m_new = jnp.maximum(m_old, jnp.maximum(z0, z1))
        keep = jnp.exp(m_old - m_new)
        e0 = jnp.exp(z0 - m_new)
        e1 = jnp.exp(z1 - m_new)
        base = (me * local_vocab + t * TILE).astype(jnp.float32)
        dist = tgt_b[...] - base
        lane = lax.broadcasted_iota(jnp.int32, (batch, 128), 1).astype(jnp.float32)
        m_l[...] = m_new
        s_l[...] = s_l[...] * keep + (e0 + e1)
        g_l[...] = g_l[...] * keep + (jnp.where(lane <= dist, e0, 0.0) + jnp.where(lane + 128.0 <= dist, e1, 0.0))

    tile(jnp.int32(0), True)
    pl.semaphore_wait(barrier, n_vp - 1)
    send_far(0)
    send(0, mate, 0).start()

    num, den = PACE

    def step(t, carry):
        tile(t, False)
        now, before = (t * num) // den, ((t - 1) * num) // den

        @pl.when(now > before)
        def _():
            send_far(now)
        send(t, mate, 0).start()
        return carry

    lax.fori_loop(1, n_tiles, step, 0)

    m_lane = m_l[...]
    m_dev = jnp.max(m_lane, axis=1, keepdims=True)
    w_lane = jnp.exp(m_lane - m_dev)
    s_dev = jnp.sum(s_l[...] * w_lane, axis=1, keepdims=True)
    g_dev = jnp.sum(g_l[...] * w_lane, axis=1, keepdims=True)
    lane = lax.broadcasted_iota(jnp.int32, (batch, 128), 1)
    packed = jnp.where(lane == 0, m_dev, jnp.where(lane == 1, s_dev, jnp.where(lane == 2, g_dev, 0.0)))
    stats = packed.T[:8, :]
    st_out[...] = stats
    st_in[me] = stats

    def st_copy(peer, k):
        return pltpu.make_async_remote_copy(
            src_ref=st_out, dst_ref=st_in.at[me], send_sem=st_send.at[k], recv_sem=st_recv.at[me],
            device_id=(dp, peer), device_id_type=MESH)

    def st_wait(src):
        pltpu.make_async_remote_copy(
            src_ref=st_out, dst_ref=st_in.at[src], send_sem=st_send.at[0], recv_sem=st_recv.at[src],
            device_id=(dp, src), device_id_type=MESH).wait_recv()

    peers = ((far0, 1), (far1, 2), (mate, 0))
    for peer, k in peers:
        st_copy(peer, k).start()
    for t in range(((n_tiles - 1) * num) // den + 1, n_tiles):
        send_far(t)
    for peer, k in peers:
        st_wait(peer)

    everyone = [st_in[i] for i in range(n_vp)]
    m_all = functools.reduce(jnp.maximum, [x[0:1] for x in everyone])
    weight = [jnp.exp(x[0:1] - m_all) for x in everyone]
    s_w = [x[1:2] * w for x, w in zip(everyone, weight)]
    inv = 1.0 / functools.reduce(jnp.add, s_w)
    cdf_ref[...] = functools.reduce(jnp.add, [x[2:3] * w for x, w in zip(everyone, weight)]) * inv
    offsets, running = [], jnp.zeros_like(inv)
    for x in s_w:
        offsets.append(running * inv)
        running = running + x
    sub = lax.broadcasted_iota(jnp.int32, (128, batch), 0)
    table = jnp.zeros((128, batch), jnp.float32)
    for i, row in enumerate([m_all, inv] + offsets):
        table = jnp.where(sub == i, row, table)
    col_b[...] = table.T
    mine = col_b[pl.ds(pl.multiple_of(me * rows, rows), rows), :]
    m_col, inv_col = mine[:, 0:1], mine[:, 1:2]
    lane_r = lax.broadcasted_iota(jnp.int32, (rows, 128), 1)

    def offset(src):
        return jnp.sum(jnp.where(lane_r == src + 2, mine, 0.0), axis=1, keepdims=True)

    def finish(src, g, carry, own):
        parts = []
        for q in range(GROUP):
            t = g * GROUP + q
            if own:
                z = stage[t, pl.ds(pl.multiple_of(me * rows, rows), rows), :]
            else:
                recv(t, src).wait_recv()
                z = tab_ref[:, pl.ds(pl.multiple_of(src * local_vocab + t * TILE, TILE), TILE)]
            parts.append(jnp.exp(z - m_col) * inv_col)
        p = jnp.concatenate(parts, axis=0)
        hi = p.astype(jnp.bfloat16)
        rest = p - hi.astype(jnp.float32)
        mid = rest.astype(jnp.bfloat16)
        low = (rest - mid.astype(jnp.float32)).astype(jnp.bfloat16)
        c = jnp.dot(jnp.concatenate([hi, mid, low], axis=1), tri[...], preferred_element_type=jnp.float32)
        for q in range(GROUP):
            t = g * GROUP + q
            cq = c[q * rows:(q + 1) * rows, :]
            tab_ref[:, pl.ds(pl.multiple_of(src * local_vocab + t * TILE, TILE), TILE)] = cq + carry
            carry = carry + cq[:, TILE - 1:TILE]
        return carry

    n_groups = n_tiles // GROUP
    lax.fori_loop(0, n_groups, lambda g, c: finish(me, g, c, True), offset(me))
    lax.fori_loop(0, n_groups, lambda g, c: finish(mate, g, c, False), offset(mate))
    lax.fori_loop(0, n_groups, lambda g, c: (finish(far0, g, c[0], False), finish(far1, g, c[1], False)),
                  (offset(far0), offset(far1)))

    def drain(t, carry):
        for peer, k in peers:
            send(t, peer, k).wait_send()
        return carry

    lax.fori_loop(0, n_tiles, drain, 0)
    for peer, k in peers:
        st_copy(peer, k).wait_send()


def solution(mesh):
    n_vp = mesh.shape["vp"]

    def local_step(hidden, w_local, inv_temp, target_ids):
        batch, depth = hidden.shape
        rows = batch // n_vp
        local_vocab = w_local.shape[1]
        n_tiles = local_vocab // TILE
        f32 = jnp.float32
        vmem = pl.BlockSpec(memory_space=pltpu.VMEM)
        hbm = pl.BlockSpec(memory_space=pl.ANY)
        table, at_target = pl.pallas_call(
            functools.partial(head_kernel, n_vp, rows, n_tiles),
            out_shape=(pltpu.VMEM((rows, n_vp * local_vocab), f32),
                       jax.ShapeDtypeStruct((1, batch), f32)),
            in_specs=[hbm, hbm, vmem, vmem],
            out_specs=(vmem, vmem),
            scratch_shapes=[
                pltpu.VMEM((batch, depth), jnp.bfloat16),
                pltpu.VMEM((SLOTS, depth, TILE), jnp.bfloat16),
                pltpu.VMEM((n_tiles, batch, TILE), f32),
                pltpu.VMEM((batch, 128), f32),
                pltpu.VMEM((batch, 128), f32),
                pltpu.VMEM((batch, 128), f32),
                pltpu.VMEM((batch, 128), f32),
                pltpu.VMEM((batch, 128), f32),
                pltpu.VMEM((8, batch), f32),
                pltpu.VMEM((n_vp, 8, batch), f32),
                pltpu.VMEM((batch, 128), f32),
                pltpu.VMEM((3 * TILE, TILE), jnp.bfloat16),
                pltpu.SemaphoreType.DMA((PIECES,)),
                pltpu.SemaphoreType.DMA((PIECES,)),
                pltpu.SemaphoreType.DMA((SLOTS,)),
                pltpu.SemaphoreType.DMA((3, n_tiles)),
                pltpu.SemaphoreType.DMA((n_vp, n_tiles)),
                pltpu.SemaphoreType.DMA((3,)),
                pltpu.SemaphoreType.DMA((n_vp,)),
            ],
            compiler_params=pltpu.CompilerParams(
                collective_id=0, has_side_effects=True, vmem_limit_bytes=45 * 2**20),
        )(hidden, w_local, inv_temp[None, :], target_ids[None, :])
        return table, at_target[0]

    return jax.shard_map(
        local_step,
        mesh=mesh,
        in_specs=(P("dp", None), P(None, "vp"), P("dp"), P("dp")),
        out_specs=(P(("dp", "vp"), None), P("dp")),
        check_vma=False,
    )
```

```python
import functools
import jax
import jax.numpy as jnp
from jax import lax
from jax.experimental import pallas as pl
from jax.experimental.pallas import tpu as pltpu
from jax.sharding import PartitionSpec as P

TILE = 256
SLOTS = 3
PIECES = 4
PACE = (3, 6, 4)
GROUP = 4
MESH = pl.DeviceIdType.MESH


def head_kernel(
    n_vp, rows, n_tiles,
    h_hbm, w_hbm, temp_hbm, tgt_hbm,
    tab_ref, cdf_ref,
    h_buf, w_buf, temp_ref, tgt_ref, stage, temp_b, tgt_b, m_l, s_l, g_l, st_out, st_in, col_b, tri,
    in_sem, h_sem, w0_sem, w_sem, half_send, half_recv, send_sem, recv_sem, st_send, st_recv,
):
    dp = lax.axis_index("dp")
    me = lax.axis_index("vp")
    batch = n_vp * rows
    local_vocab = n_tiles * TILE
    chip = me // 2
    mate = chip * 2 + lax.rem(me + 1, 2)
    far0 = (1 - chip) * 2 + lax.rem(me, 2)
    far1 = (1 - chip) * 2 + lax.rem(me + 1, 2)

    barrier = pltpu.get_barrier_semaphore()
    for peer in (mate, far0, far1):
        pl.semaphore_signal(barrier, inc=1, device_id=(dp, peer), device_id_type=MESH)

    depth = h_buf.shape[1]
    piece = depth // PIECES

    def w_copy(t):
        slot = lax.rem(t, SLOTS)
        return pltpu.make_async_copy(
            w_hbm.at[:, pl.ds(pl.multiple_of(t * TILE, TILE), TILE)], w_buf.at[slot], w_sem.at[slot])

    near = pl.multiple_of(chip * 2 * rows, 2 * rows)
    far = pl.multiple_of((1 - chip) * 2 * rows, 2 * rows)

    def h_copy(part, i):
        span = pl.ds(i * piece, piece)
        block = pl.ds(far if part == 0 else near, 2 * rows)
        return pltpu.make_async_copy(h_hbm.at[block, span], h_buf.at[block, span], h_sem.at[part, i])

    def w_half(part, i):
        span, cols = pl.ds(i * piece, piece), pl.ds(part * 128, 128)
        return pltpu.make_async_copy(w_hbm.at[span, cols], w_buf.at[0, span, cols], w0_sem.at[part, i])

    for i in range(PIECES):
        w_half(0, i).start()
        h_copy(0, i).start()
    small = (pltpu.make_async_copy(temp_hbm, temp_ref, in_sem.at[0]),
             pltpu.make_async_copy(tgt_hbm, tgt_ref, in_sem.at[1]))
    for copy in small:
        copy.start()
    for i in range(PIECES):
        w_half(1, i).start()
    for i in range(PIECES):
        h_copy(1, i).start()
    for t in range(1, SLOTS):
        w_copy(jnp.int32(t)).start()
    for copy in small:
        copy.wait()

    temp_b[...] = jnp.broadcast_to(temp_ref[...], (128, batch)).T
    tgt_b[...] = jnp.broadcast_to(tgt_ref[...].astype(jnp.float32), (128, batch)).T
    m_l[...] = jnp.full_like(m_l, -jnp.inf)
    s_l[...] = jnp.zeros_like(s_l)
    g_l[...] = jnp.zeros_like(g_l)
    r_id = lax.broadcasted_iota(jnp.int32, (TILE, TILE), 0)
    c_id = lax.broadcasted_iota(jnp.int32, (TILE, TILE), 1)
    upper = jnp.where(r_id <= c_id, 1.0, 0.0).astype(jnp.bfloat16)
    for q in range(3):
        tri[q * TILE:(q + 1) * TILE, :] = upper

    def send(t, peer, k):
        return pltpu.make_async_remote_copy(
            src_ref=stage.at[t, pl.ds(pl.multiple_of(peer * rows, rows), rows), :],
            dst_ref=tab_ref.at[:, pl.ds(pl.multiple_of(me * local_vocab + t * TILE, TILE), TILE)],
            send_sem=send_sem.at[k, t],
            recv_sem=recv_sem.at[me, t],
            device_id=(dp, peer), device_id_type=MESH)

    def recv(t, src):
        cols = tab_ref.at[:, pl.ds(pl.multiple_of(src * local_vocab + t * TILE, TILE), TILE)]
        return pltpu.make_async_remote_copy(
            src_ref=cols, dst_ref=cols, send_sem=send_sem.at[0, t], recv_sem=recv_sem.at[src, t],
            device_id=(dp, src), device_id_type=MESH)

    def send_far(t):
        send(t, far0, 1).start()
        send(t, far1, 2).start()

    def half(block, cols, part, wait_h):
        total = None
        for i in range(PIECES):
            w_half(part, i).wait()
            if wait_h:
                h_copy(0, i).wait()
            x = jnp.dot(h_buf[pl.ds(block, 2 * rows), i * piece:(i + 1) * piece],
                        w_buf[0, i * piece:(i + 1) * piece, cols], preferred_element_type=jnp.float32)
            total = x if i == 0 else total + x
        stage[0, pl.ds(block, 2 * rows), cols] = total * temp_b[pl.ds(block, 2 * rows), :]

    def send_half(part):
        cols = pl.ds(part * 128, 128)
        return [pltpu.make_async_remote_copy(
            src_ref=stage.at[0, pl.ds(pl.multiple_of(peer * rows, rows), rows), cols],
            dst_ref=tab_ref.at[:, pl.ds(pl.multiple_of(me * local_vocab + part * 128, 128), 128)],
            send_sem=half_send.at[k, part], recv_sem=half_recv.at[me, part],
            device_id=(dp, peer), device_id_type=MESH) for k, peer in enumerate((far0, far1))]

    def first_tile():
        half(far, slice(0, 128), 0, True)
        pl.semaphore_wait(barrier, n_vp - 1)
        for copy in send_half(0):
            copy.start()
        half(far, slice(128, 256), 1, False)
        total = None
        for i in range(PIECES):
            h_copy(1, i).wait()
            x = jnp.dot(h_buf[pl.ds(near, 2 * rows), i * piece:(i + 1) * piece],
                        w_buf[0, i * piece:(i + 1) * piece, :], preferred_element_type=jnp.float32)
            total = x if i == 0 else total + x
            if i == 0:
                for copy in send_half(1):
                    copy.start()
        w_copy(jnp.int32(SLOTS)).start()
        temp = temp_b[pl.ds(near, 2 * rows), :]
        stage[0, pl.ds(near, 2 * rows), :128] = total[:, :128] * temp
        stage[0, pl.ds(near, 2 * rows), 128:] = total[:, 128:] * temp
        statistics(jnp.int32(0), stage[0, :, :128], stage[0, :, 128:])

    def tile(t):
        w_copy(t).wait()
        total = jnp.dot(h_buf[...], w_buf[lax.rem(t, SLOTS)], preferred_element_type=jnp.float32)

        @pl.when(t + SLOTS < n_tiles)
        def _():
            w_copy(t + SLOTS).start()
        temp = temp_b[...]
        z0 = total[:, :128] * temp
        z1 = total[:, 128:] * temp
        stage[t, :, :128] = z0
        stage[t, :, 128:] = z1
        statistics(t, z0, z1)

    def statistics(t, z0, z1):
        m_old = m_l[...]
        m_new = jnp.maximum(m_old, jnp.maximum(z0, z1))
        keep = jnp.exp(m_old - m_new)
        e0 = jnp.exp(z0 - m_new)
        e1 = jnp.exp(z1 - m_new)
        base = (me * local_vocab + t * TILE).astype(jnp.float32)
        dist = tgt_b[...] - base
        lane = lax.broadcasted_iota(jnp.int32, (batch, 128), 1).astype(jnp.float32)
        m_l[...] = m_new
        s_l[...] = s_l[...] * keep + (e0 + e1)
        g_l[...] = g_l[...] * keep + (jnp.where(lane <= dist, e0, 0.0) + jnp.where(lane + 128.0 <= dist, e1, 0.0))

    first_tile()
    send(0, mate, 0).start()
    num, lead, den = PACE

    def started(t):
        return jnp.minimum(t, (t * num + lead) // den)

    def step(t, carry):
        tile(t)
        now = started(t)

        @pl.when(now > started(t - 1))
        def _():
            send_far(now)
        send(t, mate, 0).start()
        return carry

    lax.fori_loop(1, n_tiles, step, 0)

    m_lane = m_l[...]
    m_dev = jnp.max(m_lane, axis=1, keepdims=True)
    w_lane = jnp.exp(m_lane - m_dev)
    s_dev = jnp.sum(s_l[...] * w_lane, axis=1, keepdims=True)
    g_dev = jnp.sum(g_l[...] * w_lane, axis=1, keepdims=True)
    lane = lax.broadcasted_iota(jnp.int32, (batch, 128), 1)
    packed = jnp.where(lane == 0, m_dev, jnp.where(lane == 1, s_dev, jnp.where(lane == 2, g_dev, 0.0)))
    stats = packed.T[:8, :]
    st_out[...] = stats
    st_in[me] = stats

    def st_copy(peer, k):
        return pltpu.make_async_remote_copy(
            src_ref=st_out, dst_ref=st_in.at[me], send_sem=st_send.at[k], recv_sem=st_recv.at[me],
            device_id=(dp, peer), device_id_type=MESH)

    def st_wait(src):
        pltpu.make_async_remote_copy(
            src_ref=st_out, dst_ref=st_in.at[src], send_sem=st_send.at[0], recv_sem=st_recv.at[src],
            device_id=(dp, src), device_id_type=MESH).wait_recv()

    peers = ((far0, 1), (far1, 2), (mate, 0))
    for peer, k in peers:
        st_copy(peer, k).start()
    for t in range(min(n_tiles - 1, ((n_tiles - 1) * num + lead) // den) + 1, n_tiles):
        send_far(t)
    for peer, k in peers:
        st_wait(peer)

    everyone = [st_in[i] for i in range(n_vp)]
    m_all = functools.reduce(jnp.maximum, [x[0:1] for x in everyone])
    weight = [jnp.exp(x[0:1] - m_all) for x in everyone]
    s_w = [x[1:2] * w for x, w in zip(everyone, weight)]
    inv = 1.0 / functools.reduce(jnp.add, s_w)
    cdf_ref[...] = functools.reduce(jnp.add, [x[2:3] * w for x, w in zip(everyone, weight)]) * inv
    offsets, running = [], jnp.zeros_like(inv)
    for x in s_w:
        offsets.append(running * inv)
        running = running + x
    sub = lax.broadcasted_iota(jnp.int32, (128, batch), 0)
    table = jnp.zeros((128, batch), jnp.float32)
    for i, row in enumerate([m_all, inv] + offsets):
        table = jnp.where(sub == i, row, table)
    col_b[...] = table.T
    mine = col_b[pl.ds(pl.multiple_of(me * rows, rows), rows), :]
    m_col, inv_col = mine[:, 0:1], mine[:, 1:2]
    lane_r = lax.broadcasted_iota(jnp.int32, (rows, 128), 1)

    def offset(src):
        return jnp.sum(jnp.where(lane_r == src + 2, mine, 0.0), axis=1, keepdims=True)

    def finish(items, carries):
        carries = dict(carries)
        parts = []
        for kind, src, t in items:
            cols = pl.ds(pl.multiple_of(src * local_vocab + t * TILE, TILE), TILE)
            if kind == "own":
                z = stage[t, pl.ds(pl.multiple_of(me * rows, rows), rows), :]
            else:
                z = tab_ref[:, cols]
            parts.append(jnp.exp(z - m_col) * inv_col)
        p = jnp.concatenate(parts, axis=0)
        hi = p.astype(jnp.bfloat16)
        rest = p - hi.astype(jnp.float32)
        mid = rest.astype(jnp.bfloat16)
        low = (rest - mid.astype(jnp.float32)).astype(jnp.bfloat16)
        c = jnp.dot(jnp.concatenate([hi, mid, low], axis=1), tri[...], preferred_element_type=jnp.float32)
        for q, (kind, src, t) in enumerate(items):
            cols = pl.ds(pl.multiple_of(src * local_vocab + t * TILE, TILE), TILE)
            cq = c[q * rows:(q + 1) * rows, :]
            tab_ref[:, cols] = cq + carries[kind]
            carries[kind] = carries[kind] + cq[:, TILE - 1:TILE]
        return carries

    def run(kind, src, g, carry):
        items = [(kind, src, g * GROUP + q) for q in range(GROUP)]
        if kind != "own":
            for _, _, t in items:
                recv(t, src).wait_recv()
        return finish(items, {kind: carry})[kind]

    n_groups = n_tiles // GROUP
    lax.fori_loop(0, n_groups, lambda g, c: run("own", me, g, c), offset(me))
    lax.fori_loop(0, n_groups, lambda g, c: run("mate", mate, g, c), offset(mate))

    def far_group(g, c, first):
        out = []
        for kind, src, carry in (("far0", far0, c[0]), ("far1", far1, c[1])):
            items = [(kind, src, g * GROUP + q) for q in range(GROUP)]
            for q, (_, _, t) in enumerate(items):
                if first and q == 0:
                    for part in range(2):
                        cols = tab_ref.at[:, pl.ds(pl.multiple_of(src * local_vocab + part * 128, 128), 128)]
                        pltpu.make_async_remote_copy(
                            src_ref=cols, dst_ref=cols, send_sem=half_send.at[0, part],
                            recv_sem=half_recv.at[src, part], device_id=(dp, src), device_id_type=MESH).wait_recv()
                else:
                    recv(t, src).wait_recv()
            out.append(finish(items, {kind: carry})[kind])
        return tuple(out)

    c = far_group(0, (offset(far0), offset(far1)), True)
    c = lax.fori_loop(1, n_groups - 1, lambda g, c: far_group(g, c, False), c)

    def drain(t, carry):
        send(t, mate, 0).wait_send()
        return carry

    def drain_far(t, carry):
        send(t, far0, 1).wait_send()
        send(t, far1, 2).wait_send()
        return carry

    late = n_tiles - GROUP
    lax.fori_loop(0, n_tiles, drain, 0)
    lax.fori_loop(1, late, drain_far, 0)
    for part in range(2):
        for copy in send_half(part):
            copy.wait_send()
    for peer, k in peers:
        st_copy(peer, k).wait_send()
    carries = {"far0": c[0], "far1": c[1]}
    for t in range(late, n_tiles):
        for src in (far0, far1):
            recv(t, src).wait_recv()
        carries = finish([("far0", far0, t), ("far1", far1, t)], carries)
    lax.fori_loop(late, n_tiles, drain_far, 0)


def write_kernel(tab_ref, cdf_ref, tab_out, cdf_out, sem):
    rows = tab_ref.shape[0]
    blocks = rows // 8
    copies = [pltpu.make_async_copy(tab_ref.at[pl.ds(i * 8, 8), :], tab_out.at[pl.ds(i * 8, 8), :], sem.at[i])
              for i in range(blocks)]
    copies.append(pltpu.make_async_copy(cdf_ref, cdf_out, sem.at[blocks]))
    for copy in copies:
        copy.start()
    for copy in copies:
        copy.wait()


def solution(mesh):
    n_vp = mesh.shape["vp"]

    def local_step(hidden, w_local, inv_temp, target_ids):
        batch, depth = hidden.shape
        rows = batch // n_vp
        local_vocab = w_local.shape[1]
        n_tiles = local_vocab // TILE
        f32 = jnp.float32
        vmem = pl.BlockSpec(memory_space=pltpu.VMEM)
        hbm = pl.BlockSpec(memory_space=pl.ANY)
        table, at_target = pl.pallas_call(
            functools.partial(head_kernel, n_vp, rows, n_tiles),
            out_shape=(pltpu.VMEM((rows, n_vp * local_vocab), f32),
                       pltpu.VMEM((1, batch), f32)),
            in_specs=[hbm, hbm, hbm, hbm],
            out_specs=(vmem, vmem),
            scratch_shapes=[
                pltpu.VMEM((batch, depth), jnp.bfloat16),
                pltpu.VMEM((SLOTS, depth, TILE), jnp.bfloat16),
                pltpu.VMEM((1, batch), f32),
                pltpu.VMEM((1, batch), jnp.int32),
                pltpu.VMEM((n_tiles, batch, TILE), f32),
                pltpu.VMEM((batch, 128), f32),
                pltpu.VMEM((batch, 128), f32),
                pltpu.VMEM((batch, 128), f32),
                pltpu.VMEM((batch, 128), f32),
                pltpu.VMEM((batch, 128), f32),
                pltpu.VMEM((8, batch), f32),
                pltpu.VMEM((n_vp, 8, batch), f32),
                pltpu.VMEM((batch, 128), f32),
                pltpu.VMEM((3 * TILE, TILE), jnp.bfloat16),
                pltpu.SemaphoreType.DMA((2,)),
                pltpu.SemaphoreType.DMA((2, PIECES)),
                pltpu.SemaphoreType.DMA((2, PIECES)),
                pltpu.SemaphoreType.DMA((SLOTS,)),
                pltpu.SemaphoreType.DMA((2, 2)),
                pltpu.SemaphoreType.DMA((n_vp, 2)),
                pltpu.SemaphoreType.DMA((3, n_tiles)),
                pltpu.SemaphoreType.DMA((n_vp, n_tiles)),
                pltpu.SemaphoreType.DMA((3,)),
                pltpu.SemaphoreType.DMA((n_vp,)),
            ],
            compiler_params=pltpu.CompilerParams(
                collective_id=0, has_side_effects=True, vmem_limit_bytes=46 * 2**20),
        )(hidden, w_local, inv_temp[None, :], target_ids[None, :])
        table, at_target = pl.pallas_call(
            write_kernel,
            out_shape=(jax.ShapeDtypeStruct(table.shape, f32), jax.ShapeDtypeStruct(at_target.shape, f32)),
            in_specs=[vmem, vmem],
            out_specs=(hbm, hbm),
            scratch_shapes=[pltpu.SemaphoreType.DMA((rows // 8 + 1,))],
            compiler_params=pltpu.CompilerParams(vmem_limit_bytes=45 * 2**20),
        )(table, at_target)
        return table, at_target[0]

    return jax.shard_map(
        local_step,
        mesh=mesh,
        in_specs=(P("dp", None), P(None, "vp"), P("dp"), P("dp")),
        out_specs=(P(("dp", "vp"), None), P("dp")),
        check_vma=False,
    )
```

```python
import functools
import jax
import jax.numpy as jnp
from jax import lax
from jax.experimental import pallas as pl
from jax.experimental.pallas import tpu as pltpu
from jax.sharding import PartitionSpec as P

TILE = 256
SLOTS = 3
PIECES = 4
PACE = (3, 6, 4)
GROUP = 4
MESH = pl.DeviceIdType.MESH


def head_kernel(
    n_vp, rows, n_tiles,
    h_hbm, w_hbm, temp_hbm, tgt_hbm,
    tab_ref, cdf_ref,
    h_buf, w_buf, temp_ref, tgt_ref, stage, temp_b, tgt_b, m_l, s_l, g_l, st_out, st_in, col_b, tri,
    in_sem, h_sem, w0_sem, w_sem, half_send, half_recv, send_sem, recv_sem, st_send, st_recv,
):
    dp = lax.axis_index("dp")
    me = lax.axis_index("vp")
    batch = n_vp * rows
    local_vocab = n_tiles * TILE
    chip = me // 2
    mate = chip * 2 + lax.rem(me + 1, 2)
    far0 = (1 - chip) * 2 + lax.rem(me, 2)
    far1 = (1 - chip) * 2 + lax.rem(me + 1, 2)

    barrier = pltpu.get_barrier_semaphore()
    for peer in (mate, far0, far1):
        pl.semaphore_signal(barrier, inc=1, device_id=(dp, peer), device_id_type=MESH)

    depth = h_buf.shape[1]
    piece = depth // PIECES

    def w_copy(t):
        slot = lax.rem(t, SLOTS)
        return pltpu.make_async_copy(
            w_hbm.at[:, pl.ds(pl.multiple_of(t * TILE, TILE), TILE)], w_buf.at[slot], w_sem.at[slot])

    near = pl.multiple_of(chip * 2 * rows, 2 * rows)
    far = pl.multiple_of((1 - chip) * 2 * rows, 2 * rows)

    def h_copy(part, i):
        span = pl.ds(i * piece, piece)
        block = pl.ds(far if part == 0 else near, 2 * rows)
        return pltpu.make_async_copy(h_hbm.at[block, span], h_buf.at[block, span], h_sem.at[part, i])

    def w_half(part, i):
        span, cols = pl.ds(i * piece, piece), pl.ds(part * 128, 128)
        return pltpu.make_async_copy(w_hbm.at[span, cols], w_buf.at[0, span, cols], w0_sem.at[part, i])

    small = (pltpu.make_async_copy(temp_hbm, temp_ref, in_sem.at[0]),
             pltpu.make_async_copy(tgt_hbm, tgt_ref, in_sem.at[1]))
    for copy in small:
        copy.start()
    for i in range(PIECES):
        w_half(0, i).start(priority=1)
        h_copy(0, i).start(priority=1)
    for i in range(PIECES):
        w_half(1, i).start(priority=1)
    for i in range(PIECES):
        h_copy(1, i).start(priority=1)
    for t in range(1, SLOTS):
        w_copy(jnp.int32(t)).start(priority=1)
    for copy in small:
        copy.wait()

    temp_b[...] = jnp.broadcast_to(temp_ref[...], (128, batch)).T
    tgt_b[...] = jnp.broadcast_to(tgt_ref[...].astype(jnp.float32), (128, batch)).T
    m_l[...] = jnp.full_like(m_l, -jnp.inf)
    s_l[...] = jnp.zeros_like(s_l)
    g_l[...] = jnp.zeros_like(g_l)
    r_id = lax.broadcasted_iota(jnp.int32, (TILE, TILE), 0)
    c_id = lax.broadcasted_iota(jnp.int32, (TILE, TILE), 1)
    upper = jnp.where(r_id <= c_id, 1.0, 0.0).astype(jnp.bfloat16)
    for q in range(3):
        tri[q * TILE:(q + 1) * TILE, :] = upper

    def send(t, peer, k):
        return pltpu.make_async_remote_copy(
            src_ref=stage.at[t, pl.ds(pl.multiple_of(peer * rows, rows), rows), :],
            dst_ref=tab_ref.at[:, pl.ds(pl.multiple_of(me * local_vocab + t * TILE, TILE), TILE)],
            send_sem=send_sem.at[k, t],
            recv_sem=recv_sem.at[me, t],
            device_id=(dp, peer), device_id_type=MESH)

    def recv(t, src):
        cols = tab_ref.at[:, pl.ds(pl.multiple_of(src * local_vocab + t * TILE, TILE), TILE)]
        return pltpu.make_async_remote_copy(
            src_ref=cols, dst_ref=cols, send_sem=send_sem.at[0, t], recv_sem=recv_sem.at[src, t],
            device_id=(dp, src), device_id_type=MESH)

    def send_far(t):
        send(t, far0, 1).start()
        send(t, far1, 2).start()

    def half(block, cols, part, wait_h):
        total = None
        for i in range(PIECES):
            w_half(part, i).wait()
            if wait_h:
                h_copy(0, i).wait()
            x = jnp.dot(h_buf[pl.ds(block, 2 * rows), i * piece:(i + 1) * piece],
                        w_buf[0, i * piece:(i + 1) * piece, cols], preferred_element_type=jnp.float32)
            total = x if i == 0 else total + x
        stage[0, pl.ds(block, 2 * rows), cols] = total * temp_b[pl.ds(block, 2 * rows), :]

    def send_half(part):
        cols = pl.ds(part * 128, 128)
        return [pltpu.make_async_remote_copy(
            src_ref=stage.at[0, pl.ds(pl.multiple_of(peer * rows, rows), rows), cols],
            dst_ref=tab_ref.at[:, pl.ds(pl.multiple_of(me * local_vocab + part * 128, 128), 128)],
            send_sem=half_send.at[k, part], recv_sem=half_recv.at[me, part],
            device_id=(dp, peer), device_id_type=MESH) for k, peer in enumerate((far0, far1))]

    def first_tile():
        half(far, slice(0, 128), 0, True)
        pl.semaphore_wait(barrier, n_vp - 1)
        for copy in send_half(0):
            copy.start()
        half(far, slice(128, 256), 1, False)
        total = None
        for i in range(PIECES):
            h_copy(1, i).wait()
            x = jnp.dot(h_buf[pl.ds(near, 2 * rows), i * piece:(i + 1) * piece],
                        w_buf[0, i * piece:(i + 1) * piece, :], preferred_element_type=jnp.float32)
            total = x if i == 0 else total + x
            if i == 0:
                for copy in send_half(1):
                    copy.start()
        w_copy(jnp.int32(SLOTS)).start(priority=1)
        temp = temp_b[pl.ds(near, 2 * rows), :]
        stage[0, pl.ds(near, 2 * rows), :128] = total[:, :128] * temp
        stage[0, pl.ds(near, 2 * rows), 128:] = total[:, 128:] * temp
        statistics(jnp.int32(0), stage[0, :, :128], stage[0, :, 128:])

    def tile(t):
        w_copy(t).wait()
        total = jnp.dot(h_buf[...], w_buf[lax.rem(t, SLOTS)], preferred_element_type=jnp.float32)

        @pl.when(t + SLOTS < n_tiles)
        def _():
            w_copy(t + SLOTS).start(priority=1)
        temp = temp_b[...]
        z0 = total[:, :128] * temp
        z1 = total[:, 128:] * temp
        stage[t, :, :128] = z0
        stage[t, :, 128:] = z1
        statistics(t, z0, z1)

    def statistics(t, z0, z1):
        m_old = m_l[...]
        m_new = jnp.maximum(m_old, jnp.maximum(z0, z1))
        keep = jnp.exp(m_old - m_new)
        e0 = jnp.exp(z0 - m_new)
        e1 = jnp.exp(z1 - m_new)
        base = (me * local_vocab + t * TILE).astype(jnp.float32)
        dist = tgt_b[...] - base
        lane = lax.broadcasted_iota(jnp.int32, (batch, 128), 1).astype(jnp.float32)
        m_l[...] = m_new
        s_l[...] = s_l[...] * keep + (e0 + e1)
        g_l[...] = g_l[...] * keep + (jnp.where(lane <= dist, e0, 0.0) + jnp.where(lane + 128.0 <= dist, e1, 0.0))

    first_tile()
    send(0, mate, 0).start()
    num, lead, den = PACE

    def started(t):
        return jnp.minimum(t, (t * num + lead) // den)

    def step(t, carry):
        tile(t)
        now = started(t)

        @pl.when(now > started(t - 1))
        def _():
            send_far(now)
        send(t, mate, 0).start()
        return carry

    lax.fori_loop(1, n_tiles, step, 0)

    m_lane = m_l[...]
    m_dev = jnp.max(m_lane, axis=1, keepdims=True)
    w_lane = jnp.exp(m_lane - m_dev)
    s_dev = jnp.sum(s_l[...] * w_lane, axis=1, keepdims=True)
    g_dev = jnp.sum(g_l[...] * w_lane, axis=1, keepdims=True)
    lane = lax.broadcasted_iota(jnp.int32, (batch, 128), 1)
    packed = jnp.where(lane == 0, m_dev, jnp.where(lane == 1, s_dev, jnp.where(lane == 2, g_dev, 0.0)))
    stats = packed.T[:8, :]
    st_out[...] = stats
    st_in[me] = stats

    def st_copy(peer, k):
        return pltpu.make_async_remote_copy(
            src_ref=st_out, dst_ref=st_in.at[me], send_sem=st_send.at[k], recv_sem=st_recv.at[me],
            device_id=(dp, peer), device_id_type=MESH)

    def st_wait(src):
        pltpu.make_async_remote_copy(
            src_ref=st_out, dst_ref=st_in.at[src], send_sem=st_send.at[0], recv_sem=st_recv.at[src],
            device_id=(dp, src), device_id_type=MESH).wait_recv()

    peers = ((far0, 1), (far1, 2), (mate, 0))
    for peer, k in peers:
        st_copy(peer, k).start()
    for t in range(min(n_tiles - 1, ((n_tiles - 1) * num + lead) // den) + 1, n_tiles):
        send_far(t)
    for peer, k in peers:
        st_wait(peer)

    everyone = [st_in[i] for i in range(n_vp)]
    m_all = functools.reduce(jnp.maximum, [x[0:1] for x in everyone])
    weight = [jnp.exp(x[0:1] - m_all) for x in everyone]
    s_w = [x[1:2] * w for x, w in zip(everyone, weight)]
    inv = 1.0 / functools.reduce(jnp.add, s_w)
    cdf_ref[...] = functools.reduce(jnp.add, [x[2:3] * w for x, w in zip(everyone, weight)]) * inv
    offsets, running = [], jnp.zeros_like(inv)
    for x in s_w:
        offsets.append(running * inv)
        running = running + x
    sub = lax.broadcasted_iota(jnp.int32, (128, batch), 0)
    table = jnp.zeros((128, batch), jnp.float32)
    for i, row in enumerate([m_all, inv] + offsets):
        table = jnp.where(sub == i, row, table)
    col_b[...] = table.T
    mine = col_b[pl.ds(pl.multiple_of(me * rows, rows), rows), :]
    m_col, inv_col = mine[:, 0:1], mine[:, 1:2]
    lane_r = lax.broadcasted_iota(jnp.int32, (rows, 128), 1)

    def offset(src):
        return jnp.sum(jnp.where(lane_r == src + 2, mine, 0.0), axis=1, keepdims=True)

    def finish(items, carries):
        carries = dict(carries)
        parts = []
        for kind, src, t in items:
            cols = pl.ds(pl.multiple_of(src * local_vocab + t * TILE, TILE), TILE)
            if kind == "own":
                z = stage[t, pl.ds(pl.multiple_of(me * rows, rows), rows), :]
            else:
                z = tab_ref[:, cols]
            parts.append(jnp.exp(z - m_col) * inv_col)
        p = jnp.concatenate(parts, axis=0)
        hi = p.astype(jnp.bfloat16)
        rest = p - hi.astype(jnp.float32)
        mid = rest.astype(jnp.bfloat16)
        low = (rest - mid.astype(jnp.float32)).astype(jnp.bfloat16)
        c = jnp.dot(jnp.concatenate([hi, mid, low], axis=1), tri[...], preferred_element_type=jnp.float32)
        for q, (kind, src, t) in enumerate(items):
            cols = pl.ds(pl.multiple_of(src * local_vocab + t * TILE, TILE), TILE)
            cq = c[q * rows:(q + 1) * rows, :]
            tab_ref[:, cols] = cq + carries[kind]
            carries[kind] = carries[kind] + cq[:, TILE - 1:TILE]
        return carries

    def run(kind, src, g, carry):
        items = [(kind, src, g * GROUP + q) for q in range(GROUP)]
        if kind != "own":
            for _, _, t in items:
                recv(t, src).wait_recv()
        return finish(items, {kind: carry})[kind]

    n_groups = n_tiles // GROUP
    lax.fori_loop(0, n_groups, lambda g, c: run("own", me, g, c), offset(me))
    lax.fori_loop(0, n_groups, lambda g, c: run("mate", mate, g, c), offset(mate))

    def far_group(g, c, first):
        out = []
        for kind, src, carry in (("far0", far0, c[0]), ("far1", far1, c[1])):
            items = [(kind, src, g * GROUP + q) for q in range(GROUP)]
            for q, (_, _, t) in enumerate(items):
                if first and q == 0:
                    for part in range(2):
                        cols = tab_ref.at[:, pl.ds(pl.multiple_of(src * local_vocab + part * 128, 128), 128)]
                        pltpu.make_async_remote_copy(
                            src_ref=cols, dst_ref=cols, send_sem=half_send.at[0, part],
                            recv_sem=half_recv.at[src, part], device_id=(dp, src), device_id_type=MESH).wait_recv()
                else:
                    recv(t, src).wait_recv()
            out.append(finish(items, {kind: carry})[kind])
        return tuple(out)

    c = far_group(0, (offset(far0), offset(far1)), True)
    c = lax.fori_loop(1, n_groups - 1, lambda g, c: far_group(g, c, False), c)

    def drain(t, carry):
        send(t, mate, 0).wait_send()
        return carry

    def drain_far(t, carry):
        send(t, far0, 1).wait_send()
        send(t, far1, 2).wait_send()
        return carry

    late = n_tiles - GROUP
    lax.fori_loop(0, n_tiles, drain, 0)
    lax.fori_loop(1, late, drain_far, 0)
    for part in range(2):
        for copy in send_half(part):
            copy.wait_send()
    for peer, k in peers:
        st_copy(peer, k).wait_send()
    carries = {"far0": c[0], "far1": c[1]}
    for t in range(late, n_tiles):
        for src in (far0, far1):
            recv(t, src).wait_recv()
        carries = finish([("far0", far0, t), ("far1", far1, t)], carries)
    lax.fori_loop(late, n_tiles, drain_far, 0)


def write_kernel(tab_ref, cdf_ref, tab_out, cdf_out, sem):
    rows = tab_ref.shape[0]
    blocks = rows // 8
    copies = [pltpu.make_async_copy(tab_ref.at[pl.ds(i * 8, 8), :], tab_out.at[pl.ds(i * 8, 8), :], sem.at[i])
              for i in range(blocks)]
    copies.append(pltpu.make_async_copy(cdf_ref, cdf_out, sem.at[blocks]))
    for copy in copies:
        copy.start()
    for copy in copies:
        copy.wait()


def solution(mesh):
    n_vp = mesh.shape["vp"]

    def local_step(hidden, w_local, inv_temp, target_ids):
        batch, depth = hidden.shape
        rows = batch // n_vp
        local_vocab = w_local.shape[1]
        n_tiles = local_vocab // TILE
        f32 = jnp.float32
        vmem = pl.BlockSpec(memory_space=pltpu.VMEM)
        hbm = pl.BlockSpec(memory_space=pl.ANY)
        table, at_target = pl.pallas_call(
            functools.partial(head_kernel, n_vp, rows, n_tiles),
            out_shape=(pltpu.VMEM((rows, n_vp * local_vocab), f32),
                       pltpu.VMEM((1, batch), f32)),
            in_specs=[hbm, hbm, hbm, hbm],
            out_specs=(vmem, vmem),
            scratch_shapes=[
                pltpu.VMEM((batch, depth), jnp.bfloat16),
                pltpu.VMEM((SLOTS, depth, TILE), jnp.bfloat16),
                pltpu.VMEM((1, batch), f32),
                pltpu.VMEM((1, batch), jnp.int32),
                pltpu.VMEM((n_tiles, batch, TILE), f32),
                pltpu.VMEM((batch, 128), f32),
                pltpu.VMEM((batch, 128), f32),
                pltpu.VMEM((batch, 128), f32),
                pltpu.VMEM((batch, 128), f32),
                pltpu.VMEM((batch, 128), f32),
                pltpu.VMEM((8, batch), f32),
                pltpu.VMEM((n_vp, 8, batch), f32),
                pltpu.VMEM((batch, 128), f32),
                pltpu.VMEM((3 * TILE, TILE), jnp.bfloat16),
                pltpu.SemaphoreType.DMA((2,)),
                pltpu.SemaphoreType.DMA((2, PIECES)),
                pltpu.SemaphoreType.DMA((2, PIECES)),
                pltpu.SemaphoreType.DMA((SLOTS,)),
                pltpu.SemaphoreType.DMA((2, 2)),
                pltpu.SemaphoreType.DMA((n_vp, 2)),
                pltpu.SemaphoreType.DMA((3, n_tiles)),
                pltpu.SemaphoreType.DMA((n_vp, n_tiles)),
                pltpu.SemaphoreType.DMA((3,)),
                pltpu.SemaphoreType.DMA((n_vp,)),
            ],
            compiler_params=pltpu.CompilerParams(
                collective_id=0, has_side_effects=True, vmem_limit_bytes=46 * 2**20),
        )(hidden, w_local, inv_temp[None, :], target_ids[None, :])
        table, at_target = pl.pallas_call(
            write_kernel,
            out_shape=(jax.ShapeDtypeStruct(table.shape, f32), jax.ShapeDtypeStruct(at_target.shape, f32)),
            in_specs=[vmem, vmem],
            out_specs=(hbm, hbm),
            scratch_shapes=[pltpu.SemaphoreType.DMA((rows // 8 + 1,))],
            compiler_params=pltpu.CompilerParams(vmem_limit_bytes=45 * 2**20),
        )(table, at_target)
        return table, at_target[0]

    return jax.shard_map(
        local_step,
        mesh=mesh,
        in_specs=(P("dp", None), P(None, "vp"), P("dp"), P("dp")),
        out_specs=(P(("dp", "vp"), None), P("dp")),
        check_vma=False,
    )
```

```python
import functools
import jax
import jax.numpy as jnp
from jax import lax
from jax.experimental import pallas as pl
from jax.experimental.pallas import tpu as pltpu
from jax.sharding import PartitionSpec as P

TILE = 256
SLOTS = 3
PIECES = 4
PACE = (3, 6, 4)
GROUP = 4
MESH = pl.DeviceIdType.MESH


def head_kernel(
    n_vp, rows, n_tiles,
    h_hbm, w_hbm, temp_hbm, tgt_hbm,
    tab_ref, cdf_ref,
    h_buf, w_buf, temp_ref, tgt_ref, stage, temp_b, tgt_b, m_l, s_l, g_l, st_out, st_in, col_b, tri,
    in_sem, h_sem, w0_sem, w_sem, half_send, half_recv, send_sem, recv_sem, st_send, st_recv,
):
    dp = lax.axis_index("dp")
    me = lax.axis_index("vp")
    batch = n_vp * rows
    local_vocab = n_tiles * TILE
    chip = me // 2
    mate = chip * 2 + lax.rem(me + 1, 2)
    far0 = (1 - chip) * 2 + lax.rem(me, 2)
    far1 = (1 - chip) * 2 + lax.rem(me + 1, 2)

    barrier = pltpu.get_barrier_semaphore()
    for peer in (mate, far0, far1):
        pl.semaphore_signal(barrier, inc=1, device_id=(dp, peer), device_id_type=MESH)

    depth = h_buf.shape[1]
    piece = depth // PIECES

    def w_copy(t):
        slot = lax.rem(t, SLOTS)
        return pltpu.make_async_copy(
            w_hbm.at[:, pl.ds(pl.multiple_of(t * TILE, TILE), TILE)], w_buf.at[slot], w_sem.at[slot])

    near = pl.multiple_of(chip * 2 * rows, 2 * rows)
    far = pl.multiple_of((1 - chip) * 2 * rows, 2 * rows)

    def h_copy(part, i):
        span = pl.ds(i * piece, piece)
        block = pl.ds(far if part == 0 else near, 2 * rows)
        return pltpu.make_async_copy(h_hbm.at[block, span], h_buf.at[block, span], h_sem.at[part, i])

    def w_half(part, i):
        span, cols = pl.ds(i * piece, piece), pl.ds(0, TILE)
        return pltpu.make_async_copy(w_hbm.at[span, cols], w_buf.at[0, span, cols], w0_sem.at[part, i])

    small = (pltpu.make_async_copy(temp_hbm, temp_ref, in_sem.at[0]),
             pltpu.make_async_copy(tgt_hbm, tgt_ref, in_sem.at[1]))
    for copy in small:
        copy.start()
    for i in range(PIECES):
        w_half(0, i).start(priority=1)
        h_copy(0, i).start(priority=1)
    for i in range(PIECES):
        h_copy(1, i).start(priority=1)
    for t in range(1, SLOTS):
        w_copy(jnp.int32(t)).start(priority=1)
    for copy in small:
        copy.wait()

    temp_b[...] = jnp.broadcast_to(temp_ref[...], (128, batch)).T
    tgt_b[...] = jnp.broadcast_to(tgt_ref[...].astype(jnp.float32), (128, batch)).T
    m_l[...] = jnp.full_like(m_l, -jnp.inf)
    s_l[...] = jnp.zeros_like(s_l)
    g_l[...] = jnp.zeros_like(g_l)
    r_id = lax.broadcasted_iota(jnp.int32, (TILE, TILE), 0)
    c_id = lax.broadcasted_iota(jnp.int32, (TILE, TILE), 1)
    upper = jnp.where(r_id <= c_id, 1.0, 0.0).astype(jnp.bfloat16)
    for q in range(3):
        tri[q * TILE:(q + 1) * TILE, :] = upper

    def send(t, peer, k):
        return pltpu.make_async_remote_copy(
            src_ref=stage.at[t, pl.ds(pl.multiple_of(peer * rows, rows), rows), :],
            dst_ref=tab_ref.at[:, pl.ds(pl.multiple_of(me * local_vocab + t * TILE, TILE), TILE)],
            send_sem=send_sem.at[k, t],
            recv_sem=recv_sem.at[me, t],
            device_id=(dp, peer), device_id_type=MESH)

    def recv(t, src):
        cols = tab_ref.at[:, pl.ds(pl.multiple_of(src * local_vocab + t * TILE, TILE), TILE)]
        return pltpu.make_async_remote_copy(
            src_ref=cols, dst_ref=cols, send_sem=send_sem.at[0, t], recv_sem=recv_sem.at[src, t],
            device_id=(dp, src), device_id_type=MESH)

    def send_far(t):
        send(t, far0, 1).start()
        send(t, far1, 2).start()

    def half(block, cols, part, wait_h):
        sums = [None, None]
        for i in range(PIECES):
            if part == 0:
                w_half(part, i).wait()
            if wait_h:
                h_copy(0, i).wait()
            for q in range(2):
                span = slice(i * piece + q * piece // 2, i * piece + (q + 1) * piece // 2)
                x = jnp.dot(h_buf[pl.ds(block, 2 * rows), span], w_buf[0, span, cols],
                            preferred_element_type=jnp.float32)
                sums[q] = x if i == 0 else sums[q] + x
        temp = temp_b[pl.ds(block, 2 * rows), :]
        for c in range(0, TILE, 128):
            stage[0, pl.ds(block, 2 * rows), c:c + 128] = sums[0][:, c:c + 128] * temp + sums[1][:, c:c + 128] * temp

    def send_half(part):
        cols = pl.ds(part * 128, 128)
        return [pltpu.make_async_remote_copy(
            src_ref=stage.at[0, pl.ds(pl.multiple_of(peer * rows, rows), rows), cols],
            dst_ref=tab_ref.at[:, pl.ds(pl.multiple_of(me * local_vocab + part * 128, 128), 128)],
            send_sem=half_send.at[k, part], recv_sem=half_recv.at[me, part],
            device_id=(dp, peer), device_id_type=MESH) for k, peer in enumerate((far0, far1))]

    def first_tile():
        half(far, slice(0, TILE), 0, True)
        pl.semaphore_wait(barrier, n_vp - 1)
        for part in range(2):
            for copy in send_half(part):
                copy.start()
        sums = [None, None]
        for i in range(PIECES):
            h_copy(1, i).wait()
            for q in range(2):
                span = slice(i * piece + q * piece // 2, i * piece + (q + 1) * piece // 2)
                x = jnp.dot(h_buf[pl.ds(near, 2 * rows), span], w_buf[0, span, :],
                            preferred_element_type=jnp.float32)
                sums[q] = x if i == 0 else sums[q] + x
        w_copy(jnp.int32(SLOTS)).start(priority=1)
        temp = temp_b[pl.ds(near, 2 * rows), :]
        for c in range(0, TILE, 128):
            stage[0, pl.ds(near, 2 * rows), c:c + 128] = sums[0][:, c:c + 128] * temp + sums[1][:, c:c + 128] * temp
        statistics(jnp.int32(0), stage[0, :, :128], stage[0, :, 128:])

    def tile(t):
        w_copy(t).wait()
        total = jnp.dot(h_buf[...], w_buf[lax.rem(t, SLOTS)], preferred_element_type=jnp.float32)

        @pl.when(t + SLOTS < n_tiles)
        def _():
            w_copy(t + SLOTS).start(priority=1)
        temp = temp_b[...]
        z0 = total[:, :128] * temp
        z1 = total[:, 128:] * temp
        stage[t, :, :128] = z0
        stage[t, :, 128:] = z1
        statistics(t, z0, z1)

    def statistics(t, z0, z1):
        m_old = m_l[...]
        m_new = jnp.maximum(m_old, jnp.maximum(z0, z1))
        keep = jnp.exp(m_old - m_new)
        e0 = jnp.exp(z0 - m_new)
        e1 = jnp.exp(z1 - m_new)
        base = (me * local_vocab + t * TILE).astype(jnp.float32)
        dist = tgt_b[...] - base
        lane = lax.broadcasted_iota(jnp.int32, (batch, 128), 1).astype(jnp.float32)
        m_l[...] = m_new
        s_l[...] = s_l[...] * keep + (e0 + e1)
        g_l[...] = g_l[...] * keep + (jnp.where(lane <= dist, e0, 0.0) + jnp.where(lane + 128.0 <= dist, e1, 0.0))

    first_tile()
    send(0, mate, 0).start()
    num, lead, den = PACE

    def started(t):
        return jnp.minimum(t, (t * num + lead) // den)

    def step(t, carry):
        tile(t)
        now = started(t)

        @pl.when(now > started(t - 1))
        def _():
            send_far(now)
        send(t, mate, 0).start()
        return carry

    lax.fori_loop(1, n_tiles, step, 0)

    m_lane = m_l[...]
    m_dev = jnp.max(m_lane, axis=1, keepdims=True)
    w_lane = jnp.exp(m_lane - m_dev)
    s_dev = jnp.sum(s_l[...] * w_lane, axis=1, keepdims=True)
    g_dev = jnp.sum(g_l[...] * w_lane, axis=1, keepdims=True)
    lane = lax.broadcasted_iota(jnp.int32, (batch, 128), 1)
    packed = jnp.where(lane == 0, m_dev, jnp.where(lane == 1, s_dev, jnp.where(lane == 2, g_dev, 0.0)))
    stats = packed.T[:8, :]
    st_out[...] = stats
    st_in[me] = stats

    def st_copy(peer, k):
        return pltpu.make_async_remote_copy(
            src_ref=st_out, dst_ref=st_in.at[me], send_sem=st_send.at[k], recv_sem=st_recv.at[me],
            device_id=(dp, peer), device_id_type=MESH)

    def st_wait(src):
        pltpu.make_async_remote_copy(
            src_ref=st_out, dst_ref=st_in.at[src], send_sem=st_send.at[0], recv_sem=st_recv.at[src],
            device_id=(dp, src), device_id_type=MESH).wait_recv()

    peers = ((far0, 1), (far1, 2), (mate, 0))
    for peer, k in peers:
        st_copy(peer, k).start()
    for t in range(min(n_tiles - 1, ((n_tiles - 1) * num + lead) // den) + 1, n_tiles):
        send_far(t)
    for peer, k in peers:
        st_wait(peer)

    everyone = [st_in[i] for i in range(n_vp)]
    m_all = functools.reduce(jnp.maximum, [x[0:1] for x in everyone])
    weight = [jnp.exp(x[0:1] - m_all) for x in everyone]
    s_w = [x[1:2] * w for x, w in zip(everyone, weight)]
    inv = 1.0 / functools.reduce(jnp.add, s_w)
    cdf_ref[...] = functools.reduce(jnp.add, [x[2:3] * w for x, w in zip(everyone, weight)]) * inv
    offsets, running = [], jnp.zeros_like(inv)
    for x in s_w:
        offsets.append(running * inv)
        running = running + x
    sub = lax.broadcasted_iota(jnp.int32, (128, batch), 0)
    table = jnp.zeros((128, batch), jnp.float32)
    for i, row in enumerate([m_all, inv] + offsets):
        table = jnp.where(sub == i, row, table)
    col_b[...] = table.T
    mine = col_b[pl.ds(pl.multiple_of(me * rows, rows), rows), :]
    m_col, inv_col = mine[:, 0:1], mine[:, 1:2]
    lane_r = lax.broadcasted_iota(jnp.int32, (rows, 128), 1)

    def offset(src):
        return jnp.sum(jnp.where(lane_r == src + 2, mine, 0.0), axis=1, keepdims=True)

    def finish(items, carries):
        carries = dict(carries)
        parts = []
        for kind, src, t in items:
            cols = pl.ds(pl.multiple_of(src * local_vocab + t * TILE, TILE), TILE)
            if kind == "own":
                z = stage[t, pl.ds(pl.multiple_of(me * rows, rows), rows), :]
            else:
                z = tab_ref[:, cols]
            parts.append(jnp.exp(z - m_col) * inv_col)
        p = jnp.concatenate(parts, axis=0)
        hi = p.astype(jnp.bfloat16)
        rest = p - hi.astype(jnp.float32)
        mid = rest.astype(jnp.bfloat16)
        low = (rest - mid.astype(jnp.float32)).astype(jnp.bfloat16)
        terms = jnp.concatenate([hi, mid, low], axis=1)
        cut = p.shape[0] // 2
        c = jnp.concatenate([jnp.dot(terms[:cut], tri[...], preferred_element_type=jnp.float32),
                             jnp.dot(terms[cut:], tri[...], preferred_element_type=jnp.float32)], axis=0)
        for q, (kind, src, t) in enumerate(items):
            cols = pl.ds(pl.multiple_of(src * local_vocab + t * TILE, TILE), TILE)
            cq = c[q * rows:(q + 1) * rows, :]
            tab_ref[:, cols] = cq + carries[kind]
            carries[kind] = carries[kind] + cq[:, TILE - 1:TILE]
        return carries

    def run(kind, src, g, carry):
        items = [(kind, src, g * GROUP + q) for q in range(GROUP)]
        if kind != "own":
            for _, _, t in items:
                recv(t, src).wait_recv()
        return finish(items, {kind: carry})[kind]

    n_groups = n_tiles // GROUP
    lax.fori_loop(0, n_groups, lambda g, c: run("own", me, g, c), offset(me))
    lax.fori_loop(0, n_groups, lambda g, c: run("mate", mate, g, c), offset(mate))

    def far_group(g, c, first):
        out = []
        for kind, src, carry in (("far0", far0, c[0]), ("far1", far1, c[1])):
            items = [(kind, src, g * GROUP + q) for q in range(GROUP)]
            for q, (_, _, t) in enumerate(items):
                if first and q == 0:
                    for part in range(2):
                        cols = tab_ref.at[:, pl.ds(pl.multiple_of(src * local_vocab + part * 128, 128), 128)]
                        pltpu.make_async_remote_copy(
                            src_ref=cols, dst_ref=cols, send_sem=half_send.at[0, part],
                            recv_sem=half_recv.at[src, part], device_id=(dp, src), device_id_type=MESH).wait_recv()
                else:
                    recv(t, src).wait_recv()
            out.append(finish(items, {kind: carry})[kind])
        return tuple(out)

    c = far_group(0, (offset(far0), offset(far1)), True)
    c = lax.fori_loop(1, n_groups - 1, lambda g, c: far_group(g, c, False), c)

    def drain(t, carry):
        send(t, mate, 0).wait_send()
        return carry

    def drain_far(t, carry):
        send(t, far0, 1).wait_send()
        send(t, far1, 2).wait_send()
        return carry

    late = n_tiles - GROUP
    lax.fori_loop(0, n_tiles, drain, 0)
    lax.fori_loop(1, late, drain_far, 0)
    for part in range(2):
        for copy in send_half(part):
            copy.wait_send()
    for peer, k in peers:
        st_copy(peer, k).wait_send()
    carries = {"far0": c[0], "far1": c[1]}
    for t in range(late, n_tiles):
        for src in (far0, far1):
            recv(t, src).wait_recv()
        carries = finish([("far0", far0, t), ("far1", far1, t)], carries)
    lax.fori_loop(late, n_tiles, drain_far, 0)


def write_kernel(tab_ref, cdf_ref, tab_out, cdf_out, sem):
    rows = tab_ref.shape[0]
    blocks = rows // 8
    copies = [pltpu.make_async_copy(tab_ref.at[pl.ds(i * 8, 8), :], tab_out.at[pl.ds(i * 8, 8), :], sem.at[i])
              for i in range(blocks)]
    copies.append(pltpu.make_async_copy(cdf_ref, cdf_out, sem.at[blocks]))
    for copy in copies:
        copy.start()
    for copy in copies:
        copy.wait()


def solution(mesh):
    n_vp = mesh.shape["vp"]

    def local_step(hidden, w_local, inv_temp, target_ids):
        batch, depth = hidden.shape
        rows = batch // n_vp
        local_vocab = w_local.shape[1]
        n_tiles = local_vocab // TILE
        f32 = jnp.float32
        vmem = pl.BlockSpec(memory_space=pltpu.VMEM)
        hbm = pl.BlockSpec(memory_space=pl.ANY)
        table, at_target = pl.pallas_call(
            functools.partial(head_kernel, n_vp, rows, n_tiles),
            out_shape=(pltpu.VMEM((rows, n_vp * local_vocab), f32),
                       pltpu.VMEM((1, batch), f32)),
            in_specs=[hbm, hbm, hbm, hbm],
            out_specs=(vmem, vmem),
            scratch_shapes=[
                pltpu.VMEM((batch, depth), jnp.bfloat16),
                pltpu.VMEM((SLOTS, depth, TILE), jnp.bfloat16),
                pltpu.VMEM((1, batch), f32),
                pltpu.VMEM((1, batch), jnp.int32),
                pltpu.VMEM((n_tiles, batch, TILE), f32),
                pltpu.VMEM((batch, 128), f32),
                pltpu.VMEM((batch, 128), f32),
                pltpu.VMEM((batch, 128), f32),
                pltpu.VMEM((batch, 128), f32),
                pltpu.VMEM((batch, 128), f32),
                pltpu.VMEM((8, batch), f32),
                pltpu.VMEM((n_vp, 8, batch), f32),
                pltpu.VMEM((batch, 128), f32),
                pltpu.VMEM((3 * TILE, TILE), jnp.bfloat16),
                pltpu.SemaphoreType.DMA((2,)),
                pltpu.SemaphoreType.DMA((2, PIECES)),
                pltpu.SemaphoreType.DMA((2, PIECES)),
                pltpu.SemaphoreType.DMA((SLOTS,)),
                pltpu.SemaphoreType.DMA((2, 2)),
                pltpu.SemaphoreType.DMA((n_vp, 2)),
                pltpu.SemaphoreType.DMA((3, n_tiles)),
                pltpu.SemaphoreType.DMA((n_vp, n_tiles)),
                pltpu.SemaphoreType.DMA((3,)),
                pltpu.SemaphoreType.DMA((n_vp,)),
            ],
            compiler_params=pltpu.CompilerParams(
                collective_id=0, has_side_effects=True, vmem_limit_bytes=46 * 2**20),
        )(hidden, w_local, inv_temp[None, :], target_ids[None, :])
        table, at_target = pl.pallas_call(
            write_kernel,
            out_shape=(jax.ShapeDtypeStruct(table.shape, f32), jax.ShapeDtypeStruct(at_target.shape, f32)),
            in_specs=[vmem, vmem],
            out_specs=(hbm, hbm),
            scratch_shapes=[pltpu.SemaphoreType.DMA((rows // 8 + 1,))],
            compiler_params=pltpu.CompilerParams(vmem_limit_bytes=45 * 2**20),
        )(table, at_target)
        return table, at_target[0]

    return jax.shard_map(
        local_step,
        mesh=mesh,
        in_specs=(P("dp", None), P(None, "vp"), P("dp"), P("dp")),
        out_specs=(P(("dp", "vp"), None), P("dp")),
        check_vma=False,
    )
```
